16 devices in a mesh: prob: 2 (over y, z), feat: 8 (over x, core).
Axes of the slice: x: 4, y: 2, z: 1, core: 2. Of those that a mesh axis runs over, the one named last changes fastest.
The devices are a block of a 4x4x8 slice.
Arguments:
- design: bfloat16 [32768, 16384], P('prob', 'feat'), parts along dimension 0
- targets: float32 [32768, 200], P('prob'), parts along dimension 0
- weights_init: float32 [32768, 200], P(('prob', 'feat')), parts along dimension 0
- step_sizes: float32 [32768], P(('prob', 'feat')), parts along dimension 0
Outputs:
- output 1: float32 [32768, 200], P(('prob', 'feat')), parts along dimension 0
- output 2: float32 [32768, 200], P('prob'), parts along dimension 0
There are 2 independent parts. The reference program is written for one: setup_inputs(seed, part) draws one part's arguments, and reference() takes and returns one part's arrays. A program takes and returns all parts, laid end to end along the dimension named above; each array names one.
All inputs are finite; a program needn't handle non-finite values.
Results may differ from the reference program's by a relative error of at most 0.001.
Values are sent between devices in bfloat16 or wider.
A program may use at most 768 MiB of HBM per device.

```python
import jax
import jax.numpy as jnp
from jax import lax

SAMPLES = 16384
TARGETS = 200
FEATURES = 16384
SWEEPS = 6
SPIKE_RANK = 4
RIDGE_COEF = 1.0
MIX_WEIGHT = 0.75
STEP_TOTAL = 2.0


def spectral_bound(design, step_gain, rng_key):
    ridge_val = RIDGE_COEF / SAMPLES

    def apply_op(probe_vec):
        proj_rows = jnp.dot(design, probe_vec.astype(jnp.bfloat16), preferred_element_type=jnp.float32)
        back_cols = jnp.dot(proj_rows.astype(jnp.bfloat16), design, preferred_element_type=jnp.float32)
        return step_gain * (back_cols / SAMPLES + ridge_val * probe_vec)

    def power_step(step_idx, probe_vec):
        image_vec = apply_op(probe_vec)
        return image_vec / jnp.linalg.norm(image_vec)

    start_vec = jax.random.normal(rng_key, (FEATURES,), jnp.float32)
    probe_vec = lax.fori_loop(0, 24, power_step, start_vec / jnp.linalg.norm(start_vec))
    return jnp.linalg.norm(apply_op(probe_vec))


def setup_inputs(seed: int = 0, part: int = 0) -> dict:
    sub_keys = jax.random.split(jax.random.fold_in(jax.random.key(seed), part), 8)
    bulk_edge = (SAMPLES ** -0.5 + FEATURES ** -0.5) ** 2
    spike_amp = (2.0 * bulk_edge) ** 0.5
    noise_mat = jax.random.normal(sub_keys[0], (SAMPLES, FEATURES), jnp.float32)
    factors = jax.random.normal(sub_keys[1], (SAMPLES, SPIKE_RANK), jnp.float32)
    loadings = jax.random.normal(sub_keys[2], (SPIKE_RANK, FEATURES), jnp.float32)
    dense_x = (noise_mat + spike_amp * jnp.dot(factors, loadings)) * FEATURES ** -0.5
    design = dense_x.astype(jnp.bfloat16)
    coef_true = jax.random.normal(sub_keys[3], (FEATURES, TARGETS), jnp.float32)
    targets = jnp.dot(dense_x, coef_true) + 0.5 * jax.random.normal(sub_keys[4], (SAMPLES, TARGETS), jnp.float32)
    weights_init = jax.random.normal(sub_keys[5], (FEATURES, TARGETS), jnp.float32)
    step_gain = jax.random.uniform(sub_keys[6], (FEATURES,), jnp.float32, 0.25, 1.75)
    top_eig = spectral_bound(design, step_gain, sub_keys[7])
    step_sizes = step_gain * (STEP_TOTAL / SWEEPS) / (1.15 * top_eig)
    return {'design': design, 'targets': targets, 'weights_init': weights_init, 'step_sizes': step_sizes}


def reference(design, targets, weights_init, step_sizes):
    ridge_val = RIDGE_COEF / SAMPLES
    step_col = step_sizes[:, None]
    residual = targets - jnp.dot(design, weights_init.astype(jnp.bfloat16), preferred_element_type=jnp.float32)

    def one_sweep(state_pair, unused):
        weights, residual = state_pair
        gradient = lax.dot_general(design, residual.astype(jnp.bfloat16), (((0,), (0,)), ((), ())), preferred_element_type=jnp.float32) / SAMPLES
        update = step_col * (gradient - ridge_val * weights)
        weights = weights + MIX_WEIGHT * update
        residual = residual - MIX_WEIGHT * jnp.dot(design, update.astype(jnp.bfloat16), preferred_element_type=jnp.float32)
        return (weights, residual), None

    (weights, residual), unused_out = lax.scan(one_sweep, (weights_init, residual), None, length=SWEEPS)
    return weights, residual
```

```python
import functools

import jax
import jax.numpy as jnp
from jax import lax
from jax.experimental import pallas as pl
from jax.experimental.pallas import tpu as pltpu
from jax.sharding import PartitionSpec as P

SWEEPS = 6
RIDGE_COEF = 1.0
MIX_WEIGHT = 0.75

UNITS = 16
RING = 4
CORES = 2
DEPTH = 8
PHASES = 2 * (SWEEPS + 1)
MESH = pl.DeviceIdType.MESH

PAIR_SEND, PAIR_WAIT = 1, 2
ONE_SEND, ONE_WAIT = 3, 5
TWO_SEND, TWO_WAIT = 6, 8
NEAR_SEND, NEAR_WAIT = 9, 11
FAR_WAIT = 14
TWIN_WAIT = 16
OUT_WAIT = 17

PAIR, ONE_R, ONE_L, TWO_R, TWO_L, NEAR_R, NEAR_L, FAR_R, FAR_L, TWIN = range(10)


def _solve(targets_k, half, top, x_hbm, y_hbm, w_hbm, eta_ref, w_out, r_out,
           xbuf, contrib, pair_in, one_r, one_l, two_r, two_l, own, in1_r, in1_l, in2_r, in2_l,
           shard, gathered, gathered_f32, weights, update, gradient,
           x_sem, y_sem, w_sem, out_sem, send_sem, recv_sem):
    samples = x_hbm.shape[0]
    rows = samples // UNITS
    lanes = rows // (RING * CORES)
    low = half - top
    rest = targets_k - half
    units = PHASES * UNITS
    ridge_val = RIDGE_COEF / samples

    feat = lax.axis_index('feat')
    chip = lax.div(feat, CORES)
    core = lax.rem(feat, CORES)
    twin = 1 - core
    right = lax.rem(chip + 1 + 2 * core, RING)
    left = lax.rem(chip + 3 - 2 * core, RING)
    opposite = lax.rem(chip + 2, RING)

    def device(q, j):
        return {'feat': q * CORES + j}

    to_right, to_left, to_twin = device(right, core), device(left, core), device(chip, twin)

    barrier = pltpu.get_barrier_semaphore()
    for target in (to_right, to_left, to_twin):
        pl.semaphore_signal(barrier, inc=1, device_id=target, device_id_type=MESH)
    pl.semaphore_wait(barrier, 3)

    def remote(kind, u, src, dst, target):
        slot = lax.rem(u, DEPTH)
        return pltpu.make_async_remote_copy(
            src_ref=src, dst_ref=dst, send_sem=send_sem.at[kind, slot], recv_sem=recv_sem.at[kind, slot],
            device_id=target, device_id_type=MESH)

    def slot_of(u):
        return lax.rem(u, UNITS)

    def half_of(u):
        return lax.rem(lax.div(u, UNITS), 2)

    def pair_copy(u):
        c = slot_of(u)
        return [remote(PAIR, u, contrib.at[c, twin], pair_in.at[c], to_twin)]

    def one_copies(u):
        c = slot_of(u)
        return [remote(ONE_R, u, one_r.at[c], in1_r.at[c], to_right),
                remote(ONE_L, u, one_l.at[c], in1_l.at[c], to_left)]

    def two_copies(u):
        c = slot_of(u)
        return [remote(TWO_R, u, two_r.at[c], in2_r.at[c], to_right),
                remote(TWO_L, u, two_l.at[c], in2_l.at[c], to_left)]

    def near_copies(u, buf):
        piece = buf.at[slot_of(u), core, chip]
        return [remote(NEAR_R, u, piece, piece, to_right), remote(NEAR_L, u, piece, piece, to_left)]

    def far_copies(u, buf):
        c = slot_of(u)
        from_left = buf.at[c, core, left, pl.ds(0, top)]
        from_right = buf.at[c, core, right, pl.ds(top, low)]
        return [remote(FAR_R, u, from_left, from_left, to_right), remote(FAR_L, u, from_right, from_right, to_left)]

    def twin_copy(u, buf):
        piece = buf.at[slot_of(u), core]
        return [remote(TWIN, u, piece, piece, to_twin)]

    def out_copies(u, h):
        c = slot_of(u)
        count = half if h == 0 else rest
        copies = []
        for p in range(RING * CORES):
            start = pl.multiple_of(c * rows + p * lanes, lanes)
            copies.append(pltpu.make_async_copy(
                gathered_f32.at[c, p // RING, p % RING, pl.ds(0, count)],
                r_out.at[pl.ds(h * half, count), pl.ds(start, lanes)], out_sem.at[p]))
        return copies

    def x_copy(s):
        start = pl.multiple_of(lax.rem(s, UNITS) * rows, rows)
        return pltpu.make_async_copy(x_hbm.at[pl.ds(start, rows)], xbuf.at[lax.rem(s, 2)], x_sem.at[lax.rem(s, 2)])

    def start_all(copies):
        for copy in copies:
            copy.start()

    def wait_all(copies):
        for copy in copies:
            copy.wait()

    def stage(s, offset, action):
        u = s - offset

        @pl.when(jnp.logical_and(u >= 0, u < units))
        def _():
            action(u)

    def stage_typed(s, offset, action):
        u = s - offset
        last = units - 2 * UNITS

        @pl.when(jnp.logical_and(u >= 0, u < last))
        def _():
            action(u, gathered)

        @pl.when(jnp.logical_and(u >= last, u < units))
        def _():
            action(u, gathered_f32)

    def final_stage(s, offset, action):
        u = s - offset
        for h in range(2):
            first = units - (2 - h) * UNITS

            @pl.when(jnp.logical_and(u >= first, u < first + UNITS))
            def _():
                action(out_copies(u, h))

    def sends(s):
        stage(s, PAIR_SEND, lambda u: start_all(pair_copy(u)))
        stage(s, TWO_SEND, lambda u: start_all(two_copies(u)))
        stage_typed(s, NEAR_SEND, lambda u, buf: start_all(near_copies(u, buf)))
        stage(s, ONE_SEND, lambda u: start_all(one_copies(u)))

    def waits(s):
        def relay(u, buf):
            wait_all(near_copies(u, buf))
            start_all(far_copies(u, buf))

        def share(u, buf):
            wait_all(far_copies(u, buf))
            start_all(twin_copy(u, buf))

        stage_typed(s, NEAR_WAIT, relay)
        stage_typed(s, FAR_WAIT, share)
        stage(s, PAIR_WAIT, lambda u: wait_all(pair_copy(u)))
        stage(s, ONE_WAIT, lambda u: wait_all(one_copies(u)))
        stage(s, TWO_WAIT, lambda u: wait_all(two_copies(u)))
        stage_typed(s, TWIN_WAIT, lambda u, buf: wait_all(twin_copy(u, buf)))
        final_stage(s, OUT_WAIT, wait_all)
        final_stage(s, TWIN_WAIT, start_all)

    def reduce(s):
        c = lax.rem(s + UNITS - PAIR_WAIT, UNITS)

        def pair_sum(q, start, count):
            return contrib[c, core, q, pl.ds(start, count)] + pair_in[c, q, pl.ds(start, count)]

        one_r[c, pl.ds(0, low)] = pair_sum(opposite, top, low)
        one_r[c, pl.ds(low, top)] = pair_sum(right, 0, top)
        one_l[c, pl.ds(0, top)] = pair_sum(opposite, 0, top)
        one_l[c, pl.ds(top, low)] = pair_sum(left, top, low)
        two_r[c] = pair_sum(right, top, low)
        two_l[c] = pair_sum(left, 0, top)
        own[c] = pair_sum(chip, 0, half)

        c = lax.rem(s + UNITS - ONE_WAIT, UNITS)
        two_r[c] = two_r[c] + in1_r[c, pl.ds(0, low)]
        two_l[c] = two_l[c] + in1_l[c, pl.ds(0, top)]

        u = s - TWO_WAIT
        c = lax.rem(s + UNITS - TWO_WAIT, UNITS)
        h = lax.rem(lax.div(s + 2 * UNITS - TWO_WAIT, UNITS), 2)
        valid = jnp.logical_and(u >= 0, u < units)
        coef = jnp.where(u < 2 * UNITS, 1.0, MIX_WEIGHT).astype(jnp.float32)
        for start, count, ring_sum in (
                (0, top, in1_r[c, pl.ds(low, top)] + in2_l[c]),
                (top, low, in1_l[c, pl.ds(top, low)] + in2_r[c])):
            old = shard[h, c, pl.ds(start, count)]
            total = own[c, pl.ds(start, count)] + ring_sum
            new = jnp.where(valid, old - coef * total, old)
            shard[h, c, pl.ds(start, count)] = new
            gathered_f32[c, core, chip, pl.ds(start, count)] = new
            gathered[c, core, chip, pl.ds(start, count)] = new.astype(jnp.bfloat16)

    x_copy(0).start()
    w_copies = [
        pltpu.make_async_copy(w_hbm.at[pl.ds(0, half)], weights.at[0], w_sem.at[0]),
        pltpu.make_async_copy(w_hbm.at[pl.ds(half, rest)], weights.at[1, pl.ds(0, rest)], w_sem.at[1])]
    start_all(w_copies)

    def y_copies(c):
        start = pl.multiple_of(c * rows + (core * RING + chip) * lanes, lanes)
        return [
            pltpu.make_async_copy(y_hbm.at[pl.ds(0, half), pl.ds(start, lanes)], shard.at[0, c], y_sem.at[0, c]),
            pltpu.make_async_copy(
                y_hbm.at[pl.ds(half, rest), pl.ds(start, lanes)], shard.at[1, c, pl.ds(0, rest)], y_sem.at[1, c])]

    for c in range(UNITS):
        start_all(y_copies(c))
    if rest < half:
        weights[1, pl.ds(rest, half - rest)] = jnp.zeros((half - rest, weights.shape[2]), jnp.float32)
        shard[1, :, pl.ds(rest, half - rest)] = jnp.zeros((UNITS, half - rest, lanes), jnp.float32)
    wait_all(w_copies)
    for h in range(2):
        update[h] = weights[h].astype(jnp.bfloat16)
    for c in range(UNITS):
        wait_all(y_copies(c))

    def main_step(s, carry):
        @pl.when(s + 1 < units)
        def _():
            x_copy(s + 1).start()

        sends(s)
        waits(s)
        x_copy(s).wait()

        c = slot_of(s)
        h = half_of(s)
        x = xbuf.at[lax.rem(s, 2)]
        product = lax.dot_general(update[h], x[...], (((1,), (1,)), ((), ())), preferred_element_type=jnp.float32)
        for p in range(RING * CORES):
            contrib[c, p // RING, p % RING] = product[:, p * lanes:(p + 1) * lanes]
        residual = jnp.concatenate(
            [gathered[c, p // RING, p % RING] for p in range(RING * CORES)], axis=1)
        term = jnp.dot(residual, x[...], preferred_element_type=jnp.float32)
        gradient[...] = jnp.where(c == 0, 0.0, gradient[...]) + term
        reduce(s)

        @pl.when(jnp.logical_and(c == UNITS - 1, jnp.logical_and(s >= UNITS, s < units - UNITS)))
        def _():
            w = weights[1 - h]
            step = eta_ref[...] * (gradient[...] / samples - ridge_val * w)
            weights[1 - h] = w + MIX_WEIGHT * step
            update[1 - h] = step.astype(jnp.bfloat16)

        return carry

    lax.fori_loop(0, units, main_step, 0)

    w_copies = [
        pltpu.make_async_copy(weights.at[0], w_out.at[pl.ds(0, half)], w_sem.at[0]),
        pltpu.make_async_copy(weights.at[1, pl.ds(0, rest)], w_out.at[pl.ds(half, rest)], w_sem.at[1])]
    start_all(w_copies)

    def drain_step(s, carry):
        sends(s)
        waits(s)
        reduce(s)
        return carry

    lax.fori_loop(units, units + OUT_WAIT, drain_step, 0)
    wait_all(w_copies)


def solution(mesh):
    def local_solve(design, targets, weights, step_sizes):
        samples, depth = design.shape
        k = targets.shape[1]
        half = 8 * pl.cdiv(pl.cdiv(k, 8), 2)
        top = half // 2 // 16 * 16
        low = half - top
        rows = samples // UNITS
        lanes = rows // (RING * CORES)
        assert mesh.shape['feat'] == RING * CORES and UNITS * RING * CORES * lanes == samples
        f32, bf16 = jnp.float32, jnp.bfloat16
        hbm = pl.BlockSpec(memory_space=pl.ANY)
        w_t, r_t = pl.pallas_call(
            functools.partial(_solve, k, half, top),
            out_shape=(jax.ShapeDtypeStruct((k, depth), f32), jax.ShapeDtypeStruct((k, samples), f32)),
            in_specs=[hbm, hbm, hbm, pl.BlockSpec(memory_space=pltpu.VMEM)],
            out_specs=(hbm, hbm),
            scratch_shapes=[
                pltpu.VMEM((2, rows, depth), bf16),
                pltpu.VMEM((UNITS, CORES, RING, half, lanes), f32),
                pltpu.VMEM((UNITS, RING, half, lanes), f32),
                pltpu.VMEM((UNITS, half, lanes), f32),
                pltpu.VMEM((UNITS, half, lanes), f32),
                pltpu.VMEM((UNITS, low, lanes), f32),
                pltpu.VMEM((UNITS, top, lanes), f32),
                pltpu.VMEM((UNITS, half, lanes), f32),
                pltpu.VMEM((UNITS, half, lanes), f32),
                pltpu.VMEM((UNITS, half, lanes), f32),
                pltpu.VMEM((UNITS, low, lanes), f32),
                pltpu.VMEM((UNITS, top, lanes), f32),
                pltpu.VMEM((2, UNITS, half, lanes), f32),
                pltpu.VMEM((UNITS, CORES, RING, half, lanes), bf16),
                pltpu.VMEM((UNITS, CORES, RING, half, lanes), f32),
                pltpu.VMEM((2, half, depth), f32),
                pltpu.VMEM((2, half, depth), bf16),
                pltpu.VMEM((half, depth), f32),
                pltpu.SemaphoreType.DMA((2,)),
                pltpu.SemaphoreType.DMA((2, UNITS)),
                pltpu.SemaphoreType.DMA((2,)),
                pltpu.SemaphoreType.DMA((RING * CORES,)),
                pltpu.SemaphoreType.DMA((10, DEPTH)),
                pltpu.SemaphoreType.DMA((10, DEPTH)),
            ],
            compiler_params=pltpu.CompilerParams(
                collective_id=0, has_side_effects=True, vmem_limit_bytes=62 * 1024 * 1024),
        )(design, targets.T, weights.T, step_sizes[None, :])
        return w_t.T, r_t.T

    return jax.shard_map(
        local_solve,
        mesh=mesh,
        in_specs=(P('prob', 'feat'), P('prob', None), P(('prob', 'feat'), None), P(('prob', 'feat'))),
        out_specs=(P(('prob', 'feat'), None), P('prob', None)),
        check_vma=False,
    )
```

```python
import functools

import jax
import jax.numpy as jnp
from jax import lax
from jax.experimental import pallas as pl
from jax.experimental.pallas import tpu as pltpu
from jax.sharding import PartitionSpec as P

SWEEPS = 6
RIDGE_COEF = 1.0
MIX_WEIGHT = 0.75

UNITS = 16
RING = 4
CORES = 2
DEPTH = 8
PHASES = 2 * (SWEEPS + 1)
MESH = pl.DeviceIdType.MESH

PAIR_SEND, PAIR_WAIT = 1, 2
ONE_SEND, ONE_WAIT = 3, 5
TWO_SEND, TWO_WAIT = 6, 8
NEAR_SEND, NEAR_WAIT = 9, 11
FAR_WAIT = 14
TWIN_WAIT = 16

PAIR, ONE_R, ONE_L, TWO_R, TWO_L, NEAR_R, NEAR_L, FAR_R, FAR_L, TWIN = range(10)


def _solve(targets_k, half, top, x_hbm, y_hbm, w_hbm, eta_ref, w_out, r_out,
           xbuf, contrib, pair_in, one_r, one_l, two_r, two_l, own, in1_r, in1_l, in2_r, in2_l,
           shard, gathered, weights, update, gradient,
           x_sem, y_sem, w_sem, out_sem, send_sem, recv_sem):
    samples = x_hbm.shape[0]
    rows = samples // UNITS
    lanes = rows // (RING * CORES)
    low = half - top
    rest = targets_k - half
    units = PHASES * UNITS
    ridge_val = RIDGE_COEF / samples

    feat = lax.axis_index('feat')
    chip = lax.div(feat, CORES)
    core = lax.rem(feat, CORES)
    twin = 1 - core
    right = lax.rem(chip + 1 + 2 * core, RING)
    left = lax.rem(chip + 3 - 2 * core, RING)
    opposite = lax.rem(chip + 2, RING)

    def device(q, j):
        return {'feat': q * CORES + j}

    to_right, to_left, to_twin = device(right, core), device(left, core), device(chip, twin)

    def remote(kind, u, src, dst, target):
        slot = lax.rem(u, DEPTH)
        return pltpu.make_async_remote_copy(
            src_ref=src, dst_ref=dst, send_sem=send_sem.at[kind, slot], recv_sem=recv_sem.at[kind, slot],
            device_id=target, device_id_type=MESH)

    def slot_of(u):
        return lax.rem(u, UNITS)

    def half_of(u):
        return lax.rem(lax.div(u, UNITS), 2)

    def count_of(h):
        return half if h == 0 else rest

    def columns(c, j, q, pieces=1):
        return pl.ds(pl.multiple_of(c * rows + (j * RING + q) * lanes, lanes), pieces * lanes)

    def pair_copy(u, h):
        c, part = slot_of(u), pl.ds(0, count_of(h))
        return [remote(PAIR, u, contrib.at[c, twin, :, part], pair_in.at[c, :, part], to_twin)]

    def one_copies(u, h):
        c, part = slot_of(u), pl.ds(0, count_of(h))
        return [remote(ONE_R, u, one_r.at[c, part], in1_r.at[c, part], to_right),
                remote(ONE_L, u, one_l.at[c, part], in1_l.at[c, part], to_left)]

    def two_copies(u, h):
        c, part = slot_of(u), pl.ds(0, count_of(h) - top)
        return [remote(TWO_R, u, two_r.at[c, part], in2_r.at[c, part], to_right),
                remote(TWO_L, u, two_l.at[c], in2_l.at[c], to_left)]

    def place(u, h, last, q, start, count):
        c = slot_of(u)
        if last:
            return r_out.at[pl.ds(h * half + start, count), columns(c, core, q)]
        return gathered.at[c, core, q, pl.ds(start, count)]

    def near_copies(u, h, last):
        piece = place(u, h, last, chip, 0, count_of(h))
        source = shard.at[h, slot_of(u), pl.ds(0, count_of(h))] if last else piece
        return [remote(NEAR_R, u, source, piece, to_right), remote(NEAR_L, u, source, piece, to_left)]

    def own_copy(u, h):
        return [pltpu.make_async_copy(
            shard.at[h, slot_of(u), pl.ds(0, count_of(h))], place(u, h, True, chip, 0, count_of(h)),
            out_sem.at[lax.rem(u, DEPTH)])]

    def far_copies(u, h, last):
        from_left = place(u, h, last, left, 0, top)
        from_right = place(u, h, last, right, top, count_of(h) - top)
        return [remote(FAR_R, u, from_left, from_left, to_right), remote(FAR_L, u, from_right, from_right, to_left)]

    def twin_copy(u, h, last):
        c = slot_of(u)
        if last:
            piece = r_out.at[pl.ds(h * half, count_of(h)), columns(c, core, 0, RING)]
        else:
            piece = gathered.at[c, core, :, pl.ds(0, count_of(h))]
        return [remote(TWIN, u, piece, piece, to_twin)]

    def x_copy(s):
        start = pl.multiple_of(lax.rem(s, UNITS) * rows, rows)
        return pltpu.make_async_copy(x_hbm.at[pl.ds(start, rows)], xbuf.at[lax.rem(s, 2)], x_sem.at[lax.rem(s, 2)])

    def start_all(copies):
        for copy in copies:
            copy.start()

    def wait_all(copies):
        for copy in copies:
            copy.wait()

    def stage(s, offset, action):
        u = s - offset
        valid = jnp.logical_and(u >= 0, u < units)
        for h in range(2):
            @pl.when(jnp.logical_and(valid, half_of(u) == h))
            def _():
                action(u, h)

    def stage_typed(s, offset, action):
        u = s - offset
        final = units - 2 * UNITS
        for h in range(2):
            @pl.when(jnp.logical_and(jnp.logical_and(u >= 0, u < final), half_of(u) == h))
            def _():
                action(u, h, False)

            first = final + h * UNITS

            @pl.when(jnp.logical_and(u >= first, u < first + UNITS))
            def _():
                action(u, h, True)

    def sends(s):
        def near(u, h, last):
            start_all(near_copies(u, h, last))
            if last:
                start_all(own_copy(u, h))

        stage(s, PAIR_SEND, lambda u, h: start_all(pair_copy(u, h)))
        stage(s, TWO_SEND, lambda u, h: start_all(two_copies(u, h)))
        stage_typed(s, NEAR_SEND, near)
        stage(s, ONE_SEND, lambda u, h: start_all(one_copies(u, h)))

    def waits(s):
        def relay(u, h, last):
            wait_all(near_copies(u, h, last))
            start_all(far_copies(u, h, last))

        def share(u, h, last):
            wait_all(far_copies(u, h, last))
            if last:
                wait_all(own_copy(u, h))
            start_all(twin_copy(u, h, last))

        stage_typed(s, NEAR_WAIT, relay)
        stage_typed(s, FAR_WAIT, share)
        stage(s, PAIR_WAIT, lambda u, h: wait_all(pair_copy(u, h)))
        stage(s, ONE_WAIT, lambda u, h: wait_all(one_copies(u, h)))
        stage(s, TWO_WAIT, lambda u, h: wait_all(two_copies(u, h)))
        stage_typed(s, TWIN_WAIT, lambda u, h, last: wait_all(twin_copy(u, h, last)))

    def reduce(s):
        c = lax.rem(s + UNITS - PAIR_WAIT, UNITS)

        def pair_sum(q, start, count):
            return contrib[c, core, q, pl.ds(start, count)] + pair_in[c, q, pl.ds(start, count)]

        one_r[c, pl.ds(0, top)] = pair_sum(right, 0, top)
        one_r[c, pl.ds(top, low)] = pair_sum(opposite, top, low)
        one_l[c, pl.ds(0, top)] = pair_sum(opposite, 0, top)
        one_l[c, pl.ds(top, low)] = pair_sum(left, top, low)
        two_r[c] = pair_sum(right, top, low)
        two_l[c] = pair_sum(left, 0, top)
        own[c] = pair_sum(chip, 0, half)

        c = lax.rem(s + UNITS - ONE_WAIT, UNITS)
        two_r[c] = two_r[c] + in1_r[c, pl.ds(top, low)]
        two_l[c] = two_l[c] + in1_l[c, pl.ds(0, top)]

        u = s - TWO_WAIT
        c = lax.rem(s + UNITS - TWO_WAIT, UNITS)
        h = lax.rem(lax.div(s + 2 * UNITS - TWO_WAIT, UNITS), 2)
        valid = jnp.logical_and(u >= 0, u < units)
        coef = jnp.where(u < 2 * UNITS, 1.0, MIX_WEIGHT).astype(jnp.float32)
        for start, count, ring_sum in (
                (0, top, in1_r[c, pl.ds(0, top)] + in2_l[c]),
                (top, low, in1_l[c, pl.ds(top, low)] + in2_r[c])):
            old = shard[h, c, pl.ds(start, count)]
            total = own[c, pl.ds(start, count)] + ring_sum
            new = jnp.where(valid, old - coef * total, old)
            shard[h, c, pl.ds(start, count)] = new
            gathered[c, core, chip, pl.ds(start, count)] = new.astype(jnp.bfloat16)

    x_copy(0).start()
    w_copies = [
        pltpu.make_async_copy(w_hbm.at[pl.ds(0, half)], weights.at[0], w_sem.at[0]),
        pltpu.make_async_copy(w_hbm.at[pl.ds(half, rest)], weights.at[1, pl.ds(0, rest)], w_sem.at[1])]
    start_all(w_copies)

    def y_copies(c):
        start = pl.multiple_of(c * rows + (core * RING + chip) * lanes, lanes)
        return [
            pltpu.make_async_copy(y_hbm.at[pl.ds(0, half), pl.ds(start, lanes)], shard.at[0, c], y_sem.at[0, c]),
            pltpu.make_async_copy(
                y_hbm.at[pl.ds(half, rest), pl.ds(start, lanes)], shard.at[1, c, pl.ds(0, rest)], y_sem.at[1, c])]

    for c in range(UNITS):
        start_all(y_copies(c))
    if rest < half:
        weights[1, pl.ds(rest, half - rest)] = jnp.zeros((half - rest, weights.shape[2]), jnp.float32)
        shard[1, :, pl.ds(rest, half - rest)] = jnp.zeros((UNITS, half - rest, lanes), jnp.float32)
    barrier = pltpu.get_barrier_semaphore()
    for target in (to_right, to_left, to_twin):
        pl.semaphore_signal(barrier, inc=1, device_id=target, device_id_type=MESH)
    pl.semaphore_wait(barrier, 3)

    wait_all(w_copies)
    for h in range(2):
        update[h] = weights[h].astype(jnp.bfloat16)
    for c in range(UNITS):
        wait_all(y_copies(c))

    def main_step(s, carry, with_gradient):
        @pl.when(s + 1 < units)
        def _():
            x_copy(s + 1).start()

        sends(s)
        waits(s)
        x_copy(s).wait()

        c = slot_of(s)
        h = half_of(s)
        x = xbuf.at[lax.rem(s, 2)]
        product = lax.dot_general(update[h], x[...], (((1,), (1,)), ((), ())), preferred_element_type=jnp.float32)
        for p in range(RING * CORES):
            contrib[c, p // RING, p % RING] = product[:, p * lanes:(p + 1) * lanes]
        if with_gradient:
            residual = jnp.concatenate(
                [gathered[c, p // RING, p % RING] for p in range(RING * CORES)], axis=1)
            term = jnp.dot(residual, x[...], preferred_element_type=jnp.float32)
            gradient[...] = jnp.where(c == 0, 0.0, gradient[...]) + term
        reduce(s)
        if not with_gradient:
            return carry

        @pl.when(c == UNITS - 1)
        def _():
            w = weights[1 - h]
            step = eta_ref[...] * (gradient[...] / samples - ridge_val * w)
            weights[1 - h] = w + MIX_WEIGHT * step
            update[1 - h] = step.astype(jnp.bfloat16)

        return carry

    no_gradient = functools.partial(main_step, with_gradient=False)
    lax.fori_loop(0, UNITS, no_gradient, 0)
    lax.fori_loop(UNITS, units - UNITS, functools.partial(main_step, with_gradient=True), 0)
    lax.fori_loop(units - UNITS, units, no_gradient, 0)

    w_copies = [
        pltpu.make_async_copy(weights.at[0], w_out.at[pl.ds(0, half)], w_sem.at[0]),
        pltpu.make_async_copy(weights.at[1, pl.ds(0, rest)], w_out.at[pl.ds(half, rest)], w_sem.at[1])]
    start_all(w_copies)

    def drain_step(s, carry):
        sends(s)
        waits(s)
        reduce(s)
        return carry

    lax.fori_loop(units, units + TWIN_WAIT, drain_step, 0)
    wait_all(w_copies)


def _store(w_in, r_in, w_out, r_out, sems):
    parts = sems.shape[0] - 1
    width = r_in.shape[1] // parts
    copies = [pltpu.make_async_copy(w_in, w_out, sems.at[parts])]
    for p in range(parts):
        part = pl.ds(p * width, width)
        copies.append(pltpu.make_async_copy(r_in.at[:, part], r_out.at[:, part], sems.at[p]))
    for copy in copies:
        copy.start()
    for copy in copies:
        copy.wait()


def solution(mesh):
    def local_solve(design, targets, weights, step_sizes):
        samples, depth = design.shape
        k = targets.shape[1]
        half = 8 * pl.cdiv(pl.cdiv(k, 8), 2)
        top = half // 2 // 16 * 16
        low = half - top
        rows = samples // UNITS
        lanes = rows // (RING * CORES)
        assert mesh.shape['feat'] == RING * CORES and UNITS * RING * CORES * lanes == samples
        f32, bf16 = jnp.float32, jnp.bfloat16
        hbm = pl.BlockSpec(memory_space=pltpu.HBM)
        anywhere = pl.BlockSpec(memory_space=pl.ANY)
        w_t, r_t = pl.pallas_call(
            functools.partial(_solve, k, half, top),
            out_shape=(jax.ShapeDtypeStruct((k, depth), f32), jax.ShapeDtypeStruct((k, samples), f32)),
            in_specs=[hbm, hbm, hbm, pl.BlockSpec(memory_space=pltpu.VMEM)],
            out_specs=(anywhere, anywhere),
            scratch_shapes=[
                pltpu.VMEM((2, rows, depth), bf16),
                pltpu.VMEM((UNITS, CORES, RING, half, lanes), f32),
                pltpu.VMEM((UNITS, RING, half, lanes), f32),
                pltpu.VMEM((UNITS, half, lanes), f32),
                pltpu.VMEM((UNITS, half, lanes), f32),
                pltpu.VMEM((UNITS, low, lanes), f32),
                pltpu.VMEM((UNITS, top, lanes), f32),
                pltpu.VMEM((UNITS, half, lanes), f32),
                pltpu.VMEM((UNITS, half, lanes), f32),
                pltpu.VMEM((UNITS, half, lanes), f32),
                pltpu.VMEM((UNITS, low, lanes), f32),
                pltpu.VMEM((UNITS, top, lanes), f32),
                pltpu.VMEM((2, UNITS, half, lanes), f32),
                pltpu.VMEM((UNITS, CORES, RING, half, lanes), bf16),
                pltpu.VMEM((2, half, depth), f32),
                pltpu.VMEM((2, half, depth), bf16),
                pltpu.VMEM((half, depth), f32),
                pltpu.SemaphoreType.DMA((2,)),
                pltpu.SemaphoreType.DMA((2, UNITS)),
                pltpu.SemaphoreType.DMA((2,)),
                pltpu.SemaphoreType.DMA((DEPTH,)),
                pltpu.SemaphoreType.DMA((10, DEPTH)),
                pltpu.SemaphoreType.DMA((10, DEPTH)),
            ],
            compiler_params=pltpu.CompilerParams(
                collective_id=0, has_side_effects=True, vmem_limit_bytes=36 * 1024 * 1024),
        )(design, targets.T, weights.T, step_sizes[None, :])
        w_t, r_t = pl.pallas_call(
            _store,
            out_shape=(jax.ShapeDtypeStruct((k, depth), f32), jax.ShapeDtypeStruct((k, samples), f32)),
            in_specs=[anywhere, anywhere],
            out_specs=(hbm, hbm),
            scratch_shapes=[pltpu.SemaphoreType.DMA((9,))],
            compiler_params=pltpu.CompilerParams(vmem_limit_bytes=1024 * 1024),
        )(w_t, r_t)
        return w_t.T, r_t.T

    return jax.shard_map(
        local_solve,
        mesh=mesh,
        in_specs=(P('prob', 'feat'), P('prob', None), P(('prob', 'feat'), None), P(('prob', 'feat'))),
        out_specs=(P(('prob', 'feat'), None), P('prob', None)),
        check_vma=False,
    )
```

```python
import functools

import jax
import jax.numpy as jnp
from jax import lax
from jax.experimental import pallas as pl
from jax.experimental.pallas import tpu as pltpu
from jax.sharding import PartitionSpec as P

SWEEPS = 6
RIDGE_COEF = 1.0
MIX_WEIGHT = 0.75

UNITS = 16
RING = 4
CORES = 2
DEPTH = 8
PHASES = 2 * (SWEEPS + 1)
MESH = pl.DeviceIdType.MESH

PAIR_SEND, PAIR_WAIT = 1, 2
ONE_SEND, ONE_WAIT = 3, 6
TWO_SEND, TWO_WAIT = 7, 9
NEAR_SEND, NEAR_WAIT = 10, 12
FAR_WAIT = 14
TWIN_WAIT = UNITS

PAIR, ONE_R, ONE_L, TWO_R, TWO_L, NEAR_R, NEAR_L, FAR_R, FAR_L, TWIN = range(10)


def _solve(targets_k, half, top, x_hbm, y_hbm, w_hbm, eta_hbm, w_out, r_out,
           xbuf, contrib, pair_in, one_r, one_l, two_r, two_l, own, in1_r, in1_l, in2_r, in2_l,
           shard, gathered, weights, update, gradient, eta,
           x_sem, y_sem, w_sem, out_sem, send_sem, recv_sem):
    samples = x_hbm.shape[0]
    rows = samples // UNITS
    lanes = rows // (RING * CORES)
    low = half - top
    rest = targets_k - half
    ridge_val = RIDGE_COEF / samples

    feat = lax.axis_index('feat')
    chip = lax.div(feat, CORES)
    core = lax.rem(feat, CORES)
    twin = 1 - core
    right = lax.rem(chip + 1 + 2 * core, RING)
    left = lax.rem(chip + 3 - 2 * core, RING)
    opposite = lax.rem(chip + 2, RING)

    def device(q, j):
        return {'feat': q * CORES + j}

    to_right, to_left, to_twin = device(right, core), device(left, core), device(chip, twin)

    def unit_at(step, offset):
        phase, odd, c = step
        wrapped = c < offset
        return (phase - jnp.where(wrapped, 1, 0), jnp.where(wrapped, c + (UNITS - offset), c - offset),
                jnp.where(wrapped, 1 - odd, odd))

    def remote(kind, c, src, dst, target):
        sem = jnp.where(c >= DEPTH, c - DEPTH, c)
        return pltpu.make_async_remote_copy(
            src_ref=src, dst_ref=dst, send_sem=send_sem.at[kind, sem], recv_sem=recv_sem.at[kind, sem],
            device_id=target, device_id_type=MESH)

    def count_of(h):
        return half if h == 0 else rest

    def columns(c, j, q, pieces=1):
        return pl.ds(pl.multiple_of(c * rows + (j * RING + q) * lanes, lanes), pieces * lanes)

    def pair_copy(c, h):
        part = pl.ds(0, count_of(h))
        return [remote(PAIR, c, contrib.at[c, twin, :, part], pair_in.at[c, :, part], to_twin)]

    def one_copies(c, h):
        part = pl.ds(0, count_of(h))
        return [remote(ONE_R, c, one_r.at[c, part], in1_r.at[c, part], to_right),
                remote(ONE_L, c, one_l.at[c, part], in1_l.at[c, part], to_left)]

    def two_copies(c, h):
        part = pl.ds(0, count_of(h) - top)
        return [remote(TWO_R, c, two_r.at[c, part], in2_r.at[c, part], to_right),
                remote(TWO_L, c, two_l.at[c], in2_l.at[c], to_left)]

    def place(c, h, last, q, start, count):
        if last:
            return r_out.at[pl.ds(h * half + start, count), columns(c, core, q)]
        return gathered.at[c, core, q, pl.ds(start, count)]

    def near_copies(c, h, last):
        piece = place(c, h, last, chip, 0, count_of(h))
        source = shard.at[h, c, pl.ds(0, count_of(h))] if last else piece
        return [remote(NEAR_R, c, source, piece, to_right), remote(NEAR_L, c, source, piece, to_left)]

    def own_copy(c, h):
        return [pltpu.make_async_copy(
            shard.at[h, c, pl.ds(0, count_of(h))], place(c, h, True, chip, 0, count_of(h)),
            out_sem.at[c])]

    def far_copies(c, h, last):
        from_left = place(c, h, last, left, 0, top)
        from_right = place(c, h, last, right, top, count_of(h) - top)
        return [remote(FAR_R, c, from_left, from_left, to_right), remote(FAR_L, c, from_right, from_right, to_left)]

    def twin_copy(c, h, last):
        if last:
            piece = r_out.at[pl.ds(h * half, count_of(h)), columns(c, core, 0, RING)]
        else:
            piece = gathered.at[c, core, :, pl.ds(0, count_of(h))]
        return [remote(TWIN, c, piece, piece, to_twin)]

    def x_copy(c, buf):
        start = pl.multiple_of(c * rows, rows)
        return pltpu.make_async_copy(x_hbm.at[pl.ds(start, rows)], xbuf.at[buf], x_sem.at[buf])

    def start_all(copies):
        for copy in copies:
            copy.start()

    def wait_all(copies):
        for copy in copies:
            copy.wait()

    def stage(step, offset, action):
        phase, c, odd = unit_at(step, offset)
        valid = jnp.logical_and(phase >= 0, phase < PHASES)
        for h in range(2):
            @pl.when(jnp.logical_and(valid, odd == h))
            def _():
                action(c, h)

    def stage_typed(step, offset, action):
        phase, c, odd = unit_at(step, offset)
        rounded = jnp.logical_and(phase >= 0, phase < PHASES - 2)
        for h in range(2):
            @pl.when(jnp.logical_and(rounded, odd == h))
            def _():
                action(c, h, False)

            @pl.when(phase == PHASES - 2 + h)
            def _():
                action(c, h, True)

    def exchange(step):
        def near(c, h, last):
            start_all(near_copies(c, h, last))
            if last:
                start_all(own_copy(c, h))

        def relay(c, h, last):
            wait_all(near_copies(c, h, last))
            start_all(far_copies(c, h, last))

        def share(c, h, last):
            wait_all(far_copies(c, h, last))
            if last:
                wait_all(own_copy(c, h))
            start_all(twin_copy(c, h, last))

        stage(step, PAIR_SEND, lambda c, h: start_all(pair_copy(c, h)))
        stage_typed(step, NEAR_WAIT, relay)
        stage(step, TWO_SEND, lambda c, h: start_all(two_copies(c, h)))
        stage_typed(step, NEAR_SEND, near)
        stage(step, ONE_SEND, lambda c, h: start_all(one_copies(c, h)))
        stage_typed(step, FAR_WAIT, share)
        stage(step, PAIR_WAIT, lambda c, h: wait_all(pair_copy(c, h)))
        stage(step, TWO_WAIT, lambda c, h: wait_all(two_copies(c, h)))
        stage(step, ONE_WAIT, lambda c, h: wait_all(one_copies(c, h)))
        stage_typed(step, TWIN_WAIT, lambda c, h, last: wait_all(twin_copy(c, h, last)))

    def reduce(step):
        _, c, _ = unit_at(step, PAIR_WAIT)

        def pair_sum(q, start, count):
            return contrib[c, core, q, pl.ds(start, count)] + pair_in[c, q, pl.ds(start, count)]

        one_r[c, pl.ds(0, top)] = pair_sum(right, 0, top)
        one_r[c, pl.ds(top, low)] = pair_sum(opposite, top, low)
        one_l[c, pl.ds(0, top)] = pair_sum(opposite, 0, top)
        one_l[c, pl.ds(top, low)] = pair_sum(left, top, low)
        two_r[c] = pair_sum(right, top, low)
        two_l[c] = pair_sum(left, 0, top)
        own[c] = pair_sum(chip, 0, half)

        _, c, _ = unit_at(step, ONE_WAIT)
        two_r[c] = two_r[c] + in1_r[c, pl.ds(top, low)]
        two_l[c] = two_l[c] + in1_l[c, pl.ds(0, top)]

        phase, c, h = unit_at(step, TWO_WAIT)
        valid = jnp.logical_and(phase >= 0, phase < PHASES)
        coef = jnp.where(phase < 2, 1.0, MIX_WEIGHT).astype(jnp.float32)
        for start, count, ring_sum in (
                (0, top, in1_r[c, pl.ds(0, top)] + in2_l[c]),
                (top, low, in1_l[c, pl.ds(top, low)] + in2_r[c])):
            old = shard[h, c, pl.ds(start, count)]
            total = own[c, pl.ds(start, count)] + ring_sum
            new = jnp.where(valid, old - coef * total, old)
            shard[h, c, pl.ds(start, count)] = new
            gathered[c, core, chip, pl.ds(start, count)] = new.astype(jnp.bfloat16)

    x_copy(0, 0).start()
    eta_copy = pltpu.make_async_copy(eta_hbm, eta, w_sem.at[2])
    eta_copy.start()
    w_copies = [
        pltpu.make_async_copy(w_hbm.at[pl.ds(0, half)], weights.at[0], w_sem.at[0]),
        pltpu.make_async_copy(w_hbm.at[pl.ds(half, rest)], weights.at[1, pl.ds(0, rest)], w_sem.at[1])]
    start_all(w_copies)

    def y_copies(c):
        start = pl.multiple_of(c * rows + (core * RING + chip) * lanes, lanes)
        return [
            pltpu.make_async_copy(y_hbm.at[pl.ds(0, half), pl.ds(start, lanes)], shard.at[0, c], y_sem.at[0, c]),
            pltpu.make_async_copy(
                y_hbm.at[pl.ds(half, rest), pl.ds(start, lanes)], shard.at[1, c, pl.ds(0, rest)], y_sem.at[1, c])]

    for c in range(UNITS):
        start_all(y_copies(c))
    if rest < half:
        weights[1, pl.ds(rest, half - rest)] = jnp.zeros((half - rest, weights.shape[2]), jnp.float32)
        shard[1, :, pl.ds(rest, half - rest)] = jnp.zeros((UNITS, half - rest, lanes), jnp.float32)
    barrier = pltpu.get_barrier_semaphore()
    for target in (to_right, to_left, to_twin):
        pl.semaphore_signal(barrier, inc=1, device_id=target, device_id_type=MESH)
    pl.semaphore_wait(barrier, 3)

    wait_all(w_copies)
    eta_copy.wait()
    for h in range(2):
        update[h] = weights[h].astype(jnp.bfloat16)
    for c in range(UNITS):
        wait_all(y_copies(c))

    def main_step(phase, odd, with_gradient, more, c):
        step = (phase, odd, c)
        buf = lax.rem(c, 2)

        @pl.when(c < UNITS - 1)
        def _():
            x_copy(c + 1, 1 - buf).start()

        if more:
            @pl.when(c == UNITS - 1)
            def _():
                x_copy(0, 0).start()

        exchange(step)
        x_copy(c, buf).wait()

        x = xbuf.at[buf]
        product = lax.dot_general(update[odd], x[...], (((1,), (1,)), ((), ())), preferred_element_type=jnp.float32)
        for p in range(RING * CORES):
            contrib[c, p // RING, p % RING] = product[:, p * lanes:(p + 1) * lanes]
        if with_gradient:
            residual = jnp.concatenate(
                [gathered[c, p // RING, p % RING] for p in range(RING * CORES)], axis=1)
            term = jnp.dot(residual, x[...], preferred_element_type=jnp.float32)
            gradient[...] = jnp.where(c == 0, 0.0, gradient[...]) + term
        reduce(step)

    def run(phase, odd, with_gradient, more):
        def body(c, carry):
            main_step(phase, odd, with_gradient, more, c)
            return carry

        lax.fori_loop(0, UNITS, body, 0)

    def sweep_half(phase, carry):
        odd = lax.rem(phase, 2)
        run(phase, odd, True, True)
        w = weights[1 - odd]
        change = eta[...] * (gradient[...] / samples - ridge_val * w)
        weights[1 - odd] = w + MIX_WEIGHT * change
        update[1 - odd] = change.astype(jnp.bfloat16)
        return carry

    run(0, 0, False, True)
    lax.fori_loop(1, PHASES - 1, sweep_half, 0)
    run(PHASES - 1, 1, False, False)

    w_copies = [
        pltpu.make_async_copy(weights.at[0], w_out.at[pl.ds(0, half)], w_sem.at[0]),
        pltpu.make_async_copy(weights.at[1, pl.ds(0, rest)], w_out.at[pl.ds(half, rest)], w_sem.at[1])]
    start_all(w_copies)

    def drain_step(c, carry):
        exchange((PHASES, 0, c))
        reduce((PHASES, 0, c))
        return carry

    lax.fori_loop(0, UNITS, drain_step, 0)
    wait_all(w_copies)


def _store(w_in, r_in, w_out, r_out, sems):
    parts = sems.shape[0] - 1
    width = r_in.shape[1] // parts
    copies = [pltpu.make_async_copy(w_in, w_out, sems.at[parts])]
    for p in range(parts):
        part = pl.ds(p * width, width)
        copies.append(pltpu.make_async_copy(r_in.at[:, part], r_out.at[:, part], sems.at[p]))
    for copy in copies:
        copy.start()
    for copy in copies:
        copy.wait()


def solution(mesh):
    def local_solve(design, targets, weights, step_sizes):
        samples, depth = design.shape
        k = targets.shape[1]
        half = 8 * pl.cdiv(pl.cdiv(k, 8), 2)
        top = half // 2 // 16 * 16
        low = half - top
        rows = samples // UNITS
        lanes = rows // (RING * CORES)
        assert mesh.shape['feat'] == RING * CORES and UNITS * RING * CORES * lanes == samples
        f32, bf16 = jnp.float32, jnp.bfloat16
        hbm = pl.BlockSpec(memory_space=pltpu.HBM)
        anywhere = pl.BlockSpec(memory_space=pl.ANY)
        w_t, r_t = pl.pallas_call(
            functools.partial(_solve, k, half, top),
            out_shape=(jax.ShapeDtypeStruct((k, depth), f32), jax.ShapeDtypeStruct((k, samples), f32)),
            in_specs=[hbm, hbm, hbm, hbm],
            out_specs=(anywhere, anywhere),
            scratch_shapes=[
                pltpu.VMEM((2, rows, depth), bf16),
                pltpu.VMEM((UNITS, CORES, RING, half, lanes), f32),
                pltpu.VMEM((UNITS, RING, half, lanes), f32),
                pltpu.VMEM((UNITS, half, lanes), f32),
                pltpu.VMEM((UNITS, half, lanes), f32),
                pltpu.VMEM((UNITS, low, lanes), f32),
                pltpu.VMEM((UNITS, top, lanes), f32),
                pltpu.VMEM((UNITS, half, lanes), f32),
                pltpu.VMEM((UNITS, half, lanes), f32),
                pltpu.VMEM((UNITS, half, lanes), f32),
                pltpu.VMEM((UNITS, low, lanes), f32),
                pltpu.VMEM((UNITS, top, lanes), f32),
                pltpu.VMEM((2, UNITS, half, lanes), f32),
                pltpu.VMEM((UNITS, CORES, RING, half, lanes), bf16),
                pltpu.VMEM((2, half, depth), f32),
                pltpu.VMEM((2, half, depth), bf16),
                pltpu.VMEM((half, depth), f32),
                pltpu.VMEM((1, depth), f32),
                pltpu.SemaphoreType.DMA((2,)),
                pltpu.SemaphoreType.DMA((2, UNITS)),
                pltpu.SemaphoreType.DMA((3,)),
                pltpu.SemaphoreType.DMA((UNITS,)),
                pltpu.SemaphoreType.DMA((10, DEPTH)),
                pltpu.SemaphoreType.DMA((10, DEPTH)),
            ],
            compiler_params=pltpu.CompilerParams(
                collective_id=0, has_side_effects=True, vmem_limit_bytes=36 * 1024 * 1024),
        )(design, targets.T, pltpu.with_memory_space_constraint(weights.T, pltpu.HBM),
          pltpu.with_memory_space_constraint(step_sizes[None, :], pltpu.HBM))
        w_t, r_t = pl.pallas_call(
            _store,
            out_shape=(jax.ShapeDtypeStruct((k, depth), f32), jax.ShapeDtypeStruct((k, samples), f32)),
            in_specs=[anywhere, anywhere],
            out_specs=(hbm, hbm),
            scratch_shapes=[pltpu.SemaphoreType.DMA((9,))],
            compiler_params=pltpu.CompilerParams(vmem_limit_bytes=1024 * 1024),
        )(w_t, r_t)
        return w_t.T, r_t.T

    return jax.shard_map(
        local_solve,
        mesh=mesh,
        in_specs=(P('prob', 'feat'), P('prob', None), P(('prob', 'feat'), None), P(('prob', 'feat'))),
        out_specs=(P(('prob', 'feat'), None), P('prob', None)),
        check_vma=False,
    )
```

```python
import functools

import jax
import jax.numpy as jnp
from jax import lax
from jax.experimental import pallas as pl
from jax.experimental.pallas import tpu as pltpu
from jax.sharding import PartitionSpec as P

SWEEPS = 6
RIDGE_COEF = 1.0
MIX_WEIGHT = 0.75

UNITS = 16
RING = 4
CORES = 2
DEPTH = 8
PHASES = 2 * (SWEEPS + 1)
MESH = pl.DeviceIdType.MESH

PAIR_SEND, PAIR_WAIT = 1, 2
ONE_SEND, ONE_WAIT = 3, 6
TWO_SEND, TWO_WAIT = 7, 9
NEAR_SEND, NEAR_WAIT = 10, 12
FAR_WAIT = 14
TWIN_WAIT = UNITS

PAIR, ONE_R, ONE_L, TWO_R, TWO_L, NEAR_R, NEAR_L, FAR_R, FAR_L, TWIN = range(10)


def _solve(targets_k, half, top, x_hbm, y_hbm, w_hbm, eta_hbm, w_out, r_out,
           xbuf, turned, contrib, pair_in, one_r, one_l, two_r, two_l, own, in1_r, in1_l, in2_r, in2_l,
           shard, gathered, weights, update, gradient, eta,
           x_sem, y_sem, w_sem, out_sem, send_sem, recv_sem):
    samples = x_hbm.shape[0]
    rows = samples // UNITS
    lanes = rows // (RING * CORES)
    low = half - top
    rest = targets_k - half
    ridge_val = RIDGE_COEF / samples

    feat = lax.axis_index('feat')
    chip = lax.div(feat, CORES)
    core = lax.rem(feat, CORES)
    twin = 1 - core
    right = lax.rem(chip + 1 + 2 * core, RING)
    left = lax.rem(chip + 3 - 2 * core, RING)
    opposite = lax.rem(chip + 2, RING)

    def device(q, j):
        return {'feat': q * CORES + j}

    to_right, to_left, to_twin = device(right, core), device(left, core), device(chip, twin)

    def unit_at(step, offset):
        phase, odd, c = step
        wrapped = c < offset
        return (phase - jnp.where(wrapped, 1, 0), jnp.where(wrapped, c + (UNITS - offset), c - offset),
                jnp.where(wrapped, 1 - odd, odd))

    def remote(kind, c, src, dst, target):
        sem = jnp.where(c >= DEPTH, c - DEPTH, c)
        return pltpu.make_async_remote_copy(
            src_ref=src, dst_ref=dst, send_sem=send_sem.at[kind, sem], recv_sem=recv_sem.at[kind, sem],
            device_id=target, device_id_type=MESH)

    def count_of(h):
        return half if h == 0 else rest

    def columns(c, j, q, pieces=1):
        return pl.ds(pl.multiple_of(c * rows + (j * RING + q) * lanes, lanes), pieces * lanes)

    def pair_copy(c, h):
        part = pl.ds(0, count_of(h))
        return [remote(PAIR, c, contrib.at[c, twin, :, part], pair_in.at[c, :, part], to_twin)]

    def one_copies(c, h):
        part = pl.ds(0, count_of(h))
        return [remote(ONE_R, c, one_r.at[c, part], in1_r.at[c, part], to_right),
                remote(ONE_L, c, one_l.at[c, part], in1_l.at[c, part], to_left)]

    def two_copies(c, h):
        part = pl.ds(0, count_of(h) - top)
        return [remote(TWO_R, c, two_r.at[c, part], in2_r.at[c, part], to_right),
                remote(TWO_L, c, two_l.at[c], in2_l.at[c], to_left)]

    def place(c, h, last, q, start, count):
        if last:
            return r_out.at[pl.ds(h * half + start, count), columns(c, core, q)]
        return gathered.at[c, core, q, pl.ds(start, count)]

    def near_copies(c, h, last):
        piece = place(c, h, last, chip, 0, count_of(h))
        source = shard.at[h, c, pl.ds(0, count_of(h))] if last else piece
        return [remote(NEAR_R, c, source, piece, to_right), remote(NEAR_L, c, source, piece, to_left)]

    def own_copy(c, h):
        return [pltpu.make_async_copy(
            shard.at[h, c, pl.ds(0, count_of(h))], place(c, h, True, chip, 0, count_of(h)),
            out_sem.at[c])]

    def far_copies(c, h, last):
        from_left = place(c, h, last, left, 0, top)
        from_right = place(c, h, last, right, top, count_of(h) - top)
        return [remote(FAR_R, c, from_left, from_left, to_right), remote(FAR_L, c, from_right, from_right, to_left)]

    def twin_copy(c, h, last):
        if last:
            piece = r_out.at[pl.ds(h * half, count_of(h)), columns(c, core, 0, RING)]
        else:
            piece = gathered.at[c, core, :, pl.ds(0, count_of(h))]
        return [remote(TWIN, c, piece, piece, to_twin)]

    def x_copy(c, buf):
        start = pl.multiple_of(c * rows, rows)
        return pltpu.make_async_copy(x_hbm.at[pl.ds(start, rows)], xbuf.at[buf], x_sem.at[buf])

    def start_all(copies):
        for copy in copies:
            copy.start()

    def wait_all(copies):
        for copy in copies:
            copy.wait()

    def stage(step, offset, action):
        phase, c, odd = unit_at(step, offset)
        valid = jnp.logical_and(phase >= 0, phase < PHASES)
        for h in range(2):
            @pl.when(jnp.logical_and(valid, odd == h))
            def _():
                action(c, h)

    def stage_typed(step, offset, action):
        phase, c, odd = unit_at(step, offset)
        rounded = jnp.logical_and(phase >= 0, phase < PHASES - 2)
        for h in range(2):
            @pl.when(jnp.logical_and(rounded, odd == h))
            def _():
                action(c, h, False)

            @pl.when(phase == PHASES - 2 + h)
            def _():
                action(c, h, True)

    def exchange(step):
        def near(c, h, last):
            start_all(near_copies(c, h, last))
            if last:
                start_all(own_copy(c, h))

        def relay(c, h, last):
            wait_all(near_copies(c, h, last))
            start_all(far_copies(c, h, last))

        def share(c, h, last):
            wait_all(far_copies(c, h, last))
            if last:
                wait_all(own_copy(c, h))
            start_all(twin_copy(c, h, last))

        stage(step, PAIR_SEND, lambda c, h: start_all(pair_copy(c, h)))
        stage_typed(step, NEAR_WAIT, relay)
        stage(step, TWO_SEND, lambda c, h: start_all(two_copies(c, h)))
        stage_typed(step, NEAR_SEND, near)
        stage(step, ONE_SEND, lambda c, h: start_all(one_copies(c, h)))
        stage_typed(step, FAR_WAIT, share)
        stage(step, PAIR_WAIT, lambda c, h: wait_all(pair_copy(c, h)))
        stage(step, TWO_WAIT, lambda c, h: wait_all(two_copies(c, h)))
        stage(step, ONE_WAIT, lambda c, h: wait_all(one_copies(c, h)))
        stage_typed(step, TWIN_WAIT, lambda c, h, last: wait_all(twin_copy(c, h, last)))

    def reduce(step):
        _, c, _ = unit_at(step, PAIR_WAIT)

        def pair_sum(q, start, count):
            return contrib[c, core, q, pl.ds(start, count)] + pair_in[c, q, pl.ds(start, count)]

        one_r[c, pl.ds(0, top)] = pair_sum(right, 0, top)
        one_r[c, pl.ds(top, low)] = pair_sum(opposite, top, low)
        one_l[c, pl.ds(0, top)] = pair_sum(opposite, 0, top)
        one_l[c, pl.ds(top, low)] = pair_sum(left, top, low)
        two_r[c] = pair_sum(right, top, low)
        two_l[c] = pair_sum(left, 0, top)
        own[c] = pair_sum(chip, 0, half)

        _, c, _ = unit_at(step, ONE_WAIT)
        two_r[c] = two_r[c] + in1_r[c, pl.ds(top, low)]
        two_l[c] = two_l[c] + in1_l[c, pl.ds(0, top)]

        phase, c, h = unit_at(step, TWO_WAIT)
        valid = jnp.logical_and(phase >= 0, phase < PHASES)
        coef = jnp.where(phase < 2, 1.0, MIX_WEIGHT).astype(jnp.float32)
        for start, count, ring_sum in (
                (0, top, in1_r[c, pl.ds(0, top)] + in2_l[c]),
                (top, low, in1_l[c, pl.ds(top, low)] + in2_r[c])):
            old = shard[h, c, pl.ds(start, count)]
            total = own[c, pl.ds(start, count)] + ring_sum
            new = jnp.where(valid, old - coef * total, old)
            shard[h, c, pl.ds(start, count)] = new
            gathered[c, core, chip, pl.ds(start, count)] = new.astype(jnp.bfloat16)

    x_copy(0, 0).start()
    eta_copy = pltpu.make_async_copy(eta_hbm, eta, w_sem.at[2])
    eta_copy.start()
    w_copies = [
        pltpu.make_async_copy(w_hbm.at[pl.ds(0, half)], weights.at[0], w_sem.at[0]),
        pltpu.make_async_copy(w_hbm.at[pl.ds(half, rest)], weights.at[1, pl.ds(0, rest)], w_sem.at[1])]
    start_all(w_copies)

    def y_copies(c):
        start = pl.multiple_of(c * rows + (core * RING + chip) * lanes, lanes)
        return [
            pltpu.make_async_copy(y_hbm.at[pl.ds(0, half), pl.ds(start, lanes)], shard.at[0, c], y_sem.at[0, c]),
            pltpu.make_async_copy(
                y_hbm.at[pl.ds(half, rest), pl.ds(start, lanes)], shard.at[1, c, pl.ds(0, rest)], y_sem.at[1, c])]

    for c in range(UNITS):
        start_all(y_copies(c))
    if rest < half:
        weights[1, pl.ds(rest, half - rest)] = jnp.zeros((half - rest, weights.shape[2]), jnp.float32)
        shard[1, :, pl.ds(rest, half - rest)] = jnp.zeros((UNITS, half - rest, lanes), jnp.float32)
    barrier = pltpu.get_barrier_semaphore()
    for target in (to_right, to_left, to_twin):
        pl.semaphore_signal(barrier, inc=1, device_id=target, device_id_type=MESH)
    pl.semaphore_wait(barrier, 3)

    wait_all(w_copies)
    eta_copy.wait()
    for h in range(2):
        update[h] = weights[h].astype(jnp.bfloat16)
    for c in range(UNITS):
        wait_all(y_copies(c))

    def main_step(phase, odd, with_gradient, more, c):
        step = (phase, odd, c)
        buf = lax.rem(c, 2)

        @pl.when(c < UNITS - 1)
        def _():
            x_copy(c + 1, 1 - buf).start()

        if more:
            @pl.when(c == UNITS - 1)
            def _():
                x_copy(0, 0).start()

        exchange(step)
        x_copy(c, buf).wait()

        x = xbuf.at[buf]
        cut = rows if with_gradient else rows // 2
        if cut < rows:
            product = lax.dot_general(
                update[odd], x[pl.ds(cut, rows - cut)], (((1,), (1,)), ((), ())), preferred_element_type=jnp.float32)
            for p in range(cut // lanes, RING * CORES):
                contrib[c, p // RING, p % RING] = product[:, p * lanes - cut:(p + 1) * lanes - cut]
        turned[:, pl.ds(0, cut)] = x[pl.ds(0, cut)].T
        if with_gradient:
            residual = jnp.concatenate(
                [gathered[c, p // RING, p % RING] for p in range(RING * CORES)], axis=1)
            term = jnp.dot(residual, x[...], preferred_element_type=jnp.float32)
            gradient[...] = jnp.where(c == 0, 0.0, gradient[...]) + term
        product = jnp.dot(update[odd], turned[:, pl.ds(0, cut)], preferred_element_type=jnp.float32)
        for p in range(cut // lanes):
            contrib[c, p // RING, p % RING] = product[:, p * lanes:(p + 1) * lanes]
        reduce(step)

    def run(phase, odd, with_gradient, more):
        def body(c, carry):
            main_step(phase, odd, with_gradient, more, c)
            return carry

        lax.fori_loop(0, UNITS, body, 0)

    def sweep_half(phase, carry):
        odd = lax.rem(phase, 2)
        run(phase, odd, True, True)
        w = weights[1 - odd]
        change = eta[...] * (gradient[...] / samples - ridge_val * w)
        weights[1 - odd] = w + MIX_WEIGHT * change
        update[1 - odd] = change.astype(jnp.bfloat16)
        return carry

    run(0, 0, False, True)
    lax.fori_loop(1, PHASES - 1, sweep_half, 0)
    run(PHASES - 1, 1, False, False)

    w_copies = [
        pltpu.make_async_copy(weights.at[0], w_out.at[pl.ds(0, half)], w_sem.at[0]),
        pltpu.make_async_copy(weights.at[1, pl.ds(0, rest)], w_out.at[pl.ds(half, rest)], w_sem.at[1])]
    start_all(w_copies)

    def drain_step(c, carry):
        exchange((PHASES, 0, c))
        reduce((PHASES, 0, c))
        return carry

    lax.fori_loop(0, UNITS, drain_step, 0)
    wait_all(w_copies)


def _store(w_in, r_in, w_out, r_out, sems):
    parts = sems.shape[0] - 1
    width = r_in.shape[1] // parts
    copies = [pltpu.make_async_copy(w_in, w_out, sems.at[parts])]
    for p in range(parts):
        part = pl.ds(p * width, width)
        copies.append(pltpu.make_async_copy(r_in.at[:, part], r_out.at[:, part], sems.at[p]))
    for copy in copies:
        copy.start()
    for copy in copies:
        copy.wait()


def solution(mesh):
    def local_solve(design, targets, weights, step_sizes):
        samples, depth = design.shape
        k = targets.shape[1]
        half = 8 * pl.cdiv(pl.cdiv(k, 8), 2)
        top = half // 2 // 16 * 16
        low = half - top
        rows = samples // UNITS
        lanes = rows // (RING * CORES)
        assert mesh.shape['feat'] == RING * CORES and UNITS * RING * CORES * lanes == samples
        f32, bf16 = jnp.float32, jnp.bfloat16
        hbm = pl.BlockSpec(memory_space=pltpu.HBM)
        anywhere = pl.BlockSpec(memory_space=pl.ANY)
        w_t, r_t = pl.pallas_call(
            functools.partial(_solve, k, half, top),
            out_shape=(jax.ShapeDtypeStruct((k, depth), f32), jax.ShapeDtypeStruct((k, samples), f32)),
            in_specs=[hbm, hbm, hbm, hbm],
            out_specs=(anywhere, anywhere),
            scratch_shapes=[
                pltpu.VMEM((2, rows, depth), bf16),
                pltpu.VMEM((depth, rows), bf16),
                pltpu.VMEM((UNITS, CORES, RING, half, lanes), f32),
                pltpu.VMEM((UNITS, RING, half, lanes), f32),
                pltpu.VMEM((UNITS, half, lanes), f32),
                pltpu.VMEM((UNITS, half, lanes), f32),
                pltpu.VMEM((UNITS, low, lanes), f32),
                pltpu.VMEM((UNITS, top, lanes), f32),
                pltpu.VMEM((UNITS, half, lanes), f32),
                pltpu.VMEM((UNITS, half, lanes), f32),
                pltpu.VMEM((UNITS, half, lanes), f32),
                pltpu.VMEM((UNITS, low, lanes), f32),
                pltpu.VMEM((UNITS, top, lanes), f32),
                pltpu.VMEM((2, UNITS, half, lanes), f32),
                pltpu.VMEM((UNITS, CORES, RING, half, lanes), bf16),
                pltpu.VMEM((2, half, depth), f32),
                pltpu.VMEM((2, half, depth), bf16),
                pltpu.VMEM((half, depth), f32),
                pltpu.VMEM((1, depth), f32),
                pltpu.SemaphoreType.DMA((2,)),
                pltpu.SemaphoreType.DMA((2, UNITS)),
                pltpu.SemaphoreType.DMA((3,)),
                pltpu.SemaphoreType.DMA((UNITS,)),
                pltpu.SemaphoreType.DMA((10, DEPTH)),
                pltpu.SemaphoreType.DMA((10, DEPTH)),
            ],
            compiler_params=pltpu.CompilerParams(
                collective_id=0, has_side_effects=True, vmem_limit_bytes=39 * 1024 * 1024),
        )(design, targets.T, pltpu.with_memory_space_constraint(weights.T, pltpu.HBM),
          pltpu.with_memory_space_constraint(step_sizes[None, :], pltpu.HBM))
        w_t, r_t = pl.pallas_call(
            _store,
            out_shape=(jax.ShapeDtypeStruct((k, depth), f32), jax.ShapeDtypeStruct((k, samples), f32)),
            in_specs=[anywhere, anywhere],
            out_specs=(hbm, hbm),
            scratch_shapes=[pltpu.SemaphoreType.DMA((9,))],
            compiler_params=pltpu.CompilerParams(vmem_limit_bytes=1024 * 1024),
        )(w_t, r_t)
        return w_t.T, r_t.T

    return jax.shard_map(
        local_solve,
        mesh=mesh,
        in_specs=(P('prob', 'feat'), P('prob', None), P(('prob', 'feat'), None), P(('prob', 'feat'))),
        out_specs=(P(('prob', 'feat'), None), P('prob', None)),
        check_vma=False,
    )
```
